32 devices in a mesh: gx: 8 (over z, x), gy: 4 (over y, core).
Axes of the slice: x: 2, y: 2, z: 4, core: 2. Of those that a mesh axis runs over, the one named last changes fastest.
Arguments:
- gap_load: float32 [8, 4, 384, 128], P('gx', 'gy'), may hold values from -6 to 6
- flexibility: bfloat16 [8, 4, 768, 768], P('gx', 'gy'), as said below
- schur_blocks: bfloat16 [8, 4, 768, 768], P('gx', 'gy'), as said below
- body_modes: float32 [8, 4, 3, 768], P('gx', 'gy'), may hold values from -6 to 6
- coarse_inverse: float32 [96, 96], P(('gx', 'gy')), as said below
- saved_search: float32 [8, 4, 16, 384], P('gx', 'gy'), may hold values from -6 to 6
- saved_images: float32 [8, 4, 16, 384], P('gx', 'gy'), may hold values from -0.0068359375 to 0.0068359375
- face_slots: int32 [8, 4, 4, 192], P('gx', 'gy'), may hold values from 0 to 767, as said below
- face_count: int32 [8, 4, 4], P('gx', 'gy'), may hold values from 0 to 192, as said below
- multiplicity: int32 [8, 4, 768], P('gx', 'gy'), may hold values from 1 to 3, as said below
Outputs:
- multipliers: float32 [8, 4, 384, 128], P('gx', 'gy')
- residual: float32 [8, 4, 384, 128], P('gx', 'gy')
The draws below stay inside these ranges and needn't reach their ends.
Inputs may be any that keep to these rules, and one draw needn't show every extreme that they name: For k < face_count[a, b, d] the entries face_slots[a, b, d, k] are distinct slots of subdomain (a, b), except that faces that follow each other in the order up, right, down, left share one slot when both are not empty. Link k of the face between two neighbouring subdomains is entry k of both their lists (down of the upper one and up of the lower one, right of the left one and left of the right one). Entries with k >= face_count carry no meaning. face_count[a, b, 0] = face_count[a - 1, b, 1] and face_count[a, b, 2] = face_count[a, b - 1, 3]; faces on the grid's border have 0 links, inner faces between 96 and 192, and in every draw some face along each grid direction has exactly 192. multiplicity[a, b, i] is 1 plus the number of faces of (a, b) whose first face_count entries name slot i. `flexibility`: each block is symmetric. `schur_blocks`: each block is symmetric. `coarse_inverse`: Symmetric.
All inputs are finite; a program needn't handle non-finite values.
Results may differ from the reference program's by a relative error of at most 0.0015.
The reference program's roundings to bfloat16 on the way (of `weighted` and `lifted`) count: a program that leaves them out, or rounds other values in their place, can miss the bound.
Values sent between devices are 32-bit elements.
A program may use at most 64 MiB of HBM per device.

```python
import jax
import jax.numpy as jnp
from jax import lax

NI = 768
FACE = 192
R = 128
K = 3
NDIR = 16
ITERS = 1
SX = 8
SY = 4
NC = 96


def interface_maps(key):
    base_key = jax.random.fold_in(key, 77)
    vertical_key, horizontal_key, order_key, vertical_pick, horizontal_pick = jax.random.split(base_key, 5)
    row_index = jnp.arange(SX)[:, None]
    col_index = jnp.arange(SY)[None, :]
    vertical = jax.random.randint(vertical_key, (SX, SY), FACE // 2, FACE + 1)
    vertical = jnp.where(row_index < SX - 1, vertical, 0)
    widest = jax.random.randint(vertical_pick, (), 0, (SX - 1) * SY)
    vertical = vertical.at[widest // SY, widest % SY].set(FACE)
    horizontal = jax.random.randint(horizontal_key, (SX, SY), FACE // 2, FACE + 1)
    horizontal = jnp.where(col_index < SY - 1, horizontal, 0)
    widest_side = jax.random.randint(horizontal_pick, (), 0, SX * (SY - 1))
    horizontal = horizontal.at[widest_side // (SY - 1), widest_side % (SY - 1)].set(FACE)
    upper = jnp.concatenate([jnp.zeros((1, SY), jnp.int32), vertical[:-1]], axis=0)
    leftward = jnp.concatenate([jnp.zeros((SX, 1), jnp.int32), horizontal[:, :-1]], axis=1)
    counts = jnp.stack([upper, vertical, leftward, horizontal], axis=-1).astype(jnp.int32)
    order_keys = jax.random.split(order_key, SX * SY)
    orders = jax.vmap(lambda one_key: jax.random.permutation(one_key, NI))(order_keys).reshape(SX, SY, NI).astype(jnp.int32)
    nonempty = jnp.minimum(counts, 1)
    start_up = jnp.zeros((SX, SY), jnp.int32)
    start_right = counts[..., 0] - nonempty[..., 0] * nonempty[..., 3]
    start_down = start_right + counts[..., 3] - nonempty[..., 3] * nonempty[..., 1]
    start_left = start_down + counts[..., 1] - nonempty[..., 1] * nonempty[..., 2]
    starts = jnp.stack([start_up, start_down, start_left, start_right], axis=-1)
    position = starts[..., None] + jnp.minimum(jnp.arange(FACE, dtype=jnp.int32)[None, None, None, :], jnp.maximum(counts - 1, 0)[..., None])
    slots = jnp.take_along_axis(orders, position.reshape(SX, SY, 4 * FACE), axis=2).reshape(SX, SY, 4, FACE)
    valid = (jnp.arange(FACE)[None, None, None, :] < counts[..., None]).astype(jnp.int32)
    flat_index = (jnp.arange(SX * SY, dtype=jnp.int32)[:, None] * NI + slots.reshape(SX * SY, 4 * FACE)).reshape(-1)
    shared = jnp.zeros((SX * SY * NI,), jnp.int32).at[flat_index].add(valid.reshape(-1))
    return (slots.astype(jnp.int32), counts, (1 + shared).reshape(SX, SY, NI))


def draw_face_slots(key, part):
    return interface_maps(key)[0]


def draw_face_count(key, part):
    return interface_maps(key)[1]


def draw_multiplicity(key, part):
    return interface_maps(key)[2]


def symmetric_blocks(key, fold_tag):
    base_key = jax.random.fold_in(key, fold_tag)
    factor = 1.0 / (2.0 * jnp.sqrt(2.0 * NI))

    def one_row(row):
        row_key = jax.random.fold_in(base_key, row)
        noise_draw = jax.random.normal(row_key, (SY, NI, NI), jnp.float32)
        noise_draw = (noise_draw + jnp.swapaxes(noise_draw, 1, 2)) * factor
        return (2.0 * jnp.eye(NI, dtype=jnp.float32) + noise_draw).astype(jnp.bfloat16)
    return lax.map(one_row, jnp.arange(SX))


def draw_flexibility(key, part):
    return symmetric_blocks(key, 11)


def draw_schur_blocks(key, part):
    return symmetric_blocks(key, 12)


def draw_coarse_inverse(key, part):
    noise_key = jax.random.fold_in(key, 31)
    noise_draw = jax.random.normal(noise_key, (NC, NC), jnp.float32)
    factor = 0.3 / jnp.sqrt(2.0 * NC)
    return (jnp.eye(NC, dtype=jnp.float32) + factor * (noise_draw + noise_draw.T)) * (3.0 / NI)


def block_scale(own_key, dims, shards, smallest, largest):
    def one(axis_at, shards_of):
        steps = jax.random.uniform(jax.random.fold_in(jax.random.fold_in(own_key, 6), axis_at), (shards_of,), jnp.float32, smallest / len(shards), largest / len(shards))
        return jnp.repeat(jnp.exp(steps), dims[axis_at] // shards_of).reshape((-1,) + (1,) * (len(dims) - axis_at - 1))

    factor_of = one(*shards[0])
    for cut in shards[1:]:
        factor_of = factor_of * one(*cut)
    return factor_of


def scatter_about(stream_key, shape, deviation, reach, shards=(), kind=jnp.bfloat16):
    array = jax.random.normal(stream_key, shape, jnp.float32) * deviation
    if len(shards) > 0:
        array = block_scale(stream_key, shape, shards, -0.22, 0.18) * array
    return jnp.clip(array, min=-reach, max=reach).astype(kind)


def setup_inputs(seed: int = 0) -> dict:
    keys = jax.random.split(jax.random.key(seed), 11)
    gap_load = scatter_about(keys[0], (SX, SY, 2 * FACE, R), 1.0, 6.0, ((0, 8), (1, 4)), jnp.float32)
    flexibility = draw_flexibility(jax.random.fold_in(keys[10], 71), 0)
    schur_blocks = draw_schur_blocks(jax.random.fold_in(keys[10], 71), 0)
    body_modes = scatter_about(keys[3], (SX, SY, K, NI), 1.0, 6.0, ((0, 8), (1, 4)), jnp.float32)
    coarse_inverse = draw_coarse_inverse(jax.random.fold_in(keys[10], 71), 0)
    saved_search = scatter_about(keys[5], (SX, SY, NDIR, 2 * FACE), 1.0, 6.0, ((0, 8), (1, 4)), jnp.float32)
    saved_images = scatter_about(keys[6], (SX, SY, NDIR, 2 * FACE), (8 * FACE * SX * SY * NDIR) ** -0.5, 0.0068359375, ((0, 8), (1, 4)), jnp.float32)
    face_slots = draw_face_slots(jax.random.fold_in(keys[10], 71), 0)
    face_count = draw_face_count(jax.random.fold_in(keys[10], 71), 0)
    multiplicity = draw_multiplicity(jax.random.fold_in(keys[10], 71), 0)
    return dict(gap_load=gap_load, flexibility=flexibility, schur_blocks=schur_blocks, body_modes=body_modes, coarse_inverse=coarse_inverse, saved_search=saved_search, saved_images=saved_images, face_slots=face_slots, face_count=face_count, multiplicity=multiplicity)


HIGHEST_MODE = lax.Precision.HIGHEST


def spread(link_values, face_slots, face_valid):
    load_cases = link_values.shape[-1]
    down_links = link_values[:, :, :FACE]
    right_links = link_values[:, :, FACE:]
    from_above = jnp.concatenate([jnp.zeros_like(down_links[:1]), down_links[:-1]], axis=0)
    from_left = jnp.concatenate([jnp.zeros_like(right_links[:, :1]), right_links[:, :-1]], axis=1)
    signed_parts = jnp.stack([-from_above, down_links, -from_left, right_links], axis=2) * face_valid[..., None]

    def deposit(slot_rows, values):
        empty = jnp.zeros((NI, load_cases), values.dtype)
        return empty.at[slot_rows.reshape(-1)].add(values.reshape(-1, load_cases))

    return jax.vmap(jax.vmap(deposit))(face_slots, signed_parts)


def jumps(slot_values, face_slots, face_valid):
    load_cases = slot_values.shape[-1]

    def select(values, slot_rows):
        return values[slot_rows.reshape(-1)]

    picked = jax.vmap(jax.vmap(select))(slot_values, face_slots).reshape(SX, SY, 4, FACE, load_cases)
    from_below = jnp.concatenate([picked[1:, :, 0], jnp.zeros_like(picked[:1, :, 0])], axis=0)
    from_right = jnp.concatenate([picked[:, 1:, 2], jnp.zeros_like(picked[:, :1, 2])], axis=1)
    down_part = (picked[:, :, 1] - from_below) * face_valid[:, :, 1, :, None]
    right_part = (picked[:, :, 3] - from_right) * face_valid[:, :, 3, :, None]
    return jnp.concatenate([down_part, right_part], axis=2)


def blockwise(matrices, vectors):
    def row_block(operands):
        return jnp.einsum("bij,bjc->bic", operands[0].astype(jnp.float32), operands[1].astype(jnp.float32), precision=HIGHEST_MODE)

    return lax.map(row_block, (matrices, vectors))


def reference(gap_load, flexibility, schur_blocks, body_modes, coarse_inverse, saved_search, saved_images, face_slots, face_count, multiplicity):
    face_valid = (jnp.arange(FACE)[None, None, None, :] < face_count[..., None]).astype(jnp.float32)
    link_valid = jnp.concatenate([face_valid[:, :, 1], face_valid[:, :, 3]], axis=2)
    weights = 1.0 / multiplicity.astype(jnp.float32)
    residual = gap_load * link_valid[..., None]
    kept_search = saved_search * link_valid[:, :, None, :]
    kept_images = saved_images * link_valid[:, :, None, :]
    multipliers = jnp.zeros_like(residual)
    search_before = residual
    energy_before = jnp.ones((R,), jnp.float32)
    for iteration in range(ITERS):
        weighted = (weights[..., None] * spread(residual, face_slots, face_valid)).astype(jnp.bfloat16)
        smoothed = blockwise(schur_blocks, weighted)
        precond = jumps(weights[..., None] * smoothed, face_slots, face_valid)
        energy = jnp.sum(residual * precond, axis=(0, 1, 2))
        coarse_in = jnp.einsum("abki,abic->abkc", body_modes, spread(precond, face_slots, face_valid), precision=HIGHEST_MODE)
        coarse_out = jnp.dot(coarse_inverse, coarse_in.reshape(NC, R), precision=HIGHEST_MODE).reshape(SX, SY, K, R)
        lifted_modes = jnp.einsum("abki,abkc->abic", body_modes, coarse_out, precision=HIGHEST_MODE)
        projected = precond - jumps(lifted_modes, face_slots, face_valid)
        intersect = jnp.einsum("abjl,ablc->jc", kept_images, projected, precision=HIGHEST_MODE)
        search = projected - jnp.einsum("abjl,jc->ablc", kept_search, intersect, precision=HIGHEST_MODE)
        if iteration > 0:
            search = search + (energy / energy_before) * search_before
        lifted = spread(search, face_slots, face_valid).astype(jnp.bfloat16)
        applied = jumps(blockwise(flexibility, lifted), face_slots, face_valid)
        curvature = jnp.sum(search * applied, axis=(0, 1, 2))
        step_size = energy / curvature
        multipliers = multipliers + step_size * search
        residual = residual - step_size * applied
        search_before = search
        energy_before = energy
    return multipliers, residual
```

```python
import functools

import jax
import jax.numpy as jnp
from jax import lax
from jax.experimental import pallas as pl
from jax.experimental.pallas import tpu as pltpu
from jax.sharding import PartitionSpec as P

HIGHEST_MODE = lax.Precision.HIGHEST
MESH = pl.DeviceIdType.MESH
F32 = jnp.float32
BF16 = jnp.bfloat16
FACE_ROWS = (1, 3, 0, 2)
MODE_ROWS = 8
SLOT_ROWS = 4


def split(value):
    high = value.astype(BF16)
    return high, (value - high.astype(F32)).astype(BF16)


def wide_dot(one_hot, value):
    width = value.shape[1]
    both = jnp.concatenate(split(value), axis=1)
    out = jnp.dot(one_hot, both, preferred_element_type=F32)
    return out[:, :width] + out[:, width:]


def fine_dot(left, right):
    rows, width = left.shape[0], right.shape[1]
    lefts = jnp.concatenate(split(left), axis=0)
    rights = jnp.concatenate(split(right), axis=1)
    out = jnp.dot(lefts, rights, preferred_element_type=F32)
    return (out[:rows, :width] + out[rows:, :width]) + (out[:rows, width:] + out[rows:, width:])


def kernel(
    nx, ny,
    gap_ref, flex_hbm, schur_hbm, modes_ref, inverse_ref, search_ref, images_ref, slots_ref,
    count_ref, mult_ref,
    out_mult, out_res,
    flex, schur, gather, scatter, weight_all, modes8, inverse8, modes_out, modes_in,
    inverse_pad, inverse_in, kept_out, kept_in, gap_in, parts, parts_in, coarse_out, coarse_in,
    all_coarse, sum_y, sum_x, dir_y, dir_x, all_curv, applied, applied_in,
    load_sem, face_send, face_recv, y_send, y_recv, x_send, x_recv, all_send, all_recv,
):
    n = nx * ny
    mx = lax.axis_index("gx")
    my = lax.axis_index("gy")
    me = mx * ny + my
    slot_total = mult_ref.shape[1]
    width = slots_ref.shape[1]
    cases = gap_ref.shape[1]
    ndir = search_ref.shape[0]
    links = 4 * width
    modes = modes_ref.shape[0]
    present = (mx < nx - 1, my < ny - 1, mx > 0, my > 0)
    beside = ((mx + 1, my), (mx, my + 1), (mx - 1, my), (mx, my - 1))

    def place(index):
        return (index // ny, lax.rem(index, ny))

    load_flex = pltpu.make_async_copy(flex_hbm, flex, load_sem.at[0])
    load_schur = pltpu.make_async_copy(schur_hbm, schur, load_sem.at[1])
    load_schur.start()
    load_flex.start()

    barrier = pltpu.get_barrier_semaphore()

    def greet(step, carry):
        pl.semaphore_signal(
            barrier, inc=1, device_id=place(lax.rem(me + step, n)), device_id_type=MESH
        )
        return carry

    lax.fori_loop(1, n, greet, 0)

    def face_copy(kind, src, dst_of, face, arriving):
        landing = face if arriving else (face + 2) % 4
        return pltpu.make_async_remote_copy(
            src_ref=src, dst_ref=dst_of(landing),
            send_sem=face_send.at[kind, face], recv_sem=face_recv.at[kind, landing],
            device_id=beside[face], device_id_type=MESH,
        )

    def send_face(kind, src, dst_of, face):
        @pl.when(present[face])
        def _():
            face_copy(kind, src, dst_of, face, False).start()

    def recv_face(kind, src, dst_of, face):
        @pl.when(present[face])
        def _():
            face_copy(kind, src, dst_of, face, True).wait_recv()

    def sent_face(kind, src, dst_of, face):
        @pl.when(present[face])
        def _():
            face_copy(kind, src, dst_of, face, False).wait_send()

    def row_of(face):
        row = slots_ref[FACE_ROWS[face] : FACE_ROWS[face] + 1, :]
        at = lax.broadcasted_iota(jnp.int32, (1, width), 1)
        return jnp.where(at < count_ref[0, FACE_ROWS[face]], row, -1).astype(F32)

    slot_row = jnp.concatenate([row_of(face) for face in range(4)], axis=1)
    slot_at = lax.broadcasted_iota(jnp.int32, (slot_total, links), 0).astype(F32)
    scatter[...] = jnp.where(slot_at == slot_row, 1.0, 0.0).astype(BF16)

    modes8[...] = jnp.zeros_like(modes8)
    modes8[0:modes, :] = modes_ref[...]
    mode_parts = jnp.concatenate(split(modes8[...]), axis=0)
    rest = modes8[...] - mode_parts[:MODE_ROWS].astype(F32) - mode_parts[MODE_ROWS:].astype(F32)
    mode_parts = jnp.concatenate(
        [mode_parts[:MODE_ROWS].astype(F32), mode_parts[MODE_ROWS:].astype(F32), rest], axis=0
    ).astype(BF16)
    picked3 = jnp.dot(mode_parts, scatter[...], preferred_element_type=F32)
    picked_modes = (
        picked3[:MODE_ROWS] + picked3[MODE_ROWS : 2 * MODE_ROWS] + picked3[2 * MODE_ROWS :]
    )
    for face in range(4):
        modes_out[face] = picked_modes[:, face * width : (face + 1) * width]

    inverse8[...] = jnp.zeros_like(inverse8)
    inverse8[0:modes, :] = inverse_ref[...]
    chunk = min(n, 32)
    from_at = lax.broadcasted_iota(jnp.int32, (modes * chunk, SLOT_ROWS * chunk), 0)
    to_at = lax.broadcasted_iota(jnp.int32, (modes * chunk, SLOT_ROWS * chunk), 1)
    inner = to_at % SLOT_ROWS
    expand = jnp.where((inner < modes) & (from_at == (to_at // SLOT_ROWS) * modes + inner), 1.0, 0.0)
    for at in range(n // chunk):
        inverse_pad[:, at * SLOT_ROWS * chunk : (at + 1) * SLOT_ROWS * chunk] = jnp.dot(
            inverse8[:, at * modes * chunk : (at + 1) * modes * chunk], expand,
            precision=HIGHEST_MODE, preferred_element_type=F32,
        )

    for face in range(2):
        kept_out[face, 0:ndir, :] = search_ref[:, face * width : (face + 1) * width]
        kept_out[face, ndir:, :] = images_ref[:, face * width : (face + 1) * width]

    pl.semaphore_wait(barrier, n - 1)

    def modes_dst(face):
        return modes_in.at[face]

    def inverse_dst(face):
        return inverse_in.at[face]

    def kept_dst(face):
        return kept_in.at[face - 2]

    def gap_dst(face):
        return gap_in.at[face - 2]

    for face in range(2):
        send_face(2, kept_out.at[face], kept_dst, face)
        send_face(0, modes_out.at[face], modes_dst, face)
        send_face(1, inverse_pad, inverse_dst, face)
        send_face(3, gap_ref.at[pl.ds(face * width, width)], gap_dst, face)
    for face in range(2, 4):
        send_face(0, modes_out.at[face], modes_dst, face)
        send_face(1, inverse_pad, inverse_dst, face)

    columns = jnp.transpose(jnp.broadcast_to(slot_row, (128, links)))
    lane = lax.broadcasted_iota(jnp.int32, (links, 128), 1).astype(F32)
    for at in range(slot_total // 128):
        gather[:, at * 128 : (at + 1) * 128] = jnp.where(
            columns == lane + float(at * 128), 1.0, 0.0
        ).astype(BF16)
    weight_row = 1.0 / mult_ref[...].astype(F32)
    weight_all[...] = jnp.transpose(jnp.broadcast_to(weight_row, (cases, slot_total)))

    row_at = lax.broadcasted_iota(jnp.int32, (width, cases), 0)

    def masked(value, face):
        return jnp.where(row_at < count_ref[0, FACE_ROWS[face]], value, 0.0)

    own_gap = jnp.concatenate(
        [masked(gap_ref[face * width : (face + 1) * width, :], face) for face in range(2)], axis=0
    )
    own_spread = wide_dot(scatter[:, : 2 * width], own_gap)

    for face in range(4):
        recv_face(0, modes_out.at[face], modes_dst, face)
        recv_face(1, inverse_pad, inverse_dst, face)
    for face in range(2, 4):
        recv_face(2, kept_out.at[face - 2], kept_dst, face)

    def lanes_masked(value, face):
        at = lax.broadcasted_iota(jnp.int32, value.shape, 1)
        return jnp.where(at < count_ref[0, FACE_ROWS[face]], value, 0.0)

    near = jnp.concatenate([lanes_masked(-modes_in[face], face) for face in range(4)], axis=1)
    at = lax.broadcasted_iota(jnp.int32, near.shape, 1)
    blocks = [picked_modes]
    for face in range(4):
        blocks.append(jnp.where((at >= face * width) & (at < (face + 1) * width), near, 0.0))
    mode_rows = jnp.concatenate(blocks, axis=0)
    kept = [lanes_masked(kept_out[face], face) for face in range(2)]
    kept += [lanes_masked(-kept_in[face - 2], face) for face in range(2, 4)]
    kept = jnp.concatenate(kept, axis=1)
    kept_search, kept_images = kept[:ndir], kept[ndir:]
    measure_rows = jnp.concatenate([mode_rows, kept_images], axis=0)
    filler = jnp.zeros((128 - 5 * MODE_ROWS - ndir, links), F32)
    lift = jnp.transpose(jnp.concatenate([mode_rows, kept_search, filler], axis=0))
    lift_high, lift_low = split(lift)
    lift3 = jnp.concatenate([lift_high, lift_high, lift_low], axis=1)

    own_part = lax.dot_general(
        kept_images, picked_modes, (((1,), (1,)), ((), ())),
        precision=HIGHEST_MODE, preferred_element_type=F32,
    )
    direct = jnp.dot(
        own_part, inverse_pad[...], precision=HIGHEST_MODE, preferred_element_type=F32
    )

    def y_copy(kind, buffer, step, arriving):
        slot = lax.rem(my - step + ny, ny) if arriving else my
        return pltpu.make_async_remote_copy(
            src_ref=buffer.at[my], dst_ref=buffer.at[slot],
            send_sem=y_send.at[kind, step], recv_sem=y_recv.at[kind, step],
            device_id=(mx, lax.rem(my + step, ny)), device_id_type=MESH,
        )

    def x_copy(kind, buffer, step, arriving):
        slot = lax.rem(mx - step + nx, nx) if arriving else mx
        return pltpu.make_async_remote_copy(
            src_ref=buffer.at[mx], dst_ref=buffer.at[slot],
            send_sem=x_send.at[kind, step], recv_sem=x_recv.at[kind, step],
            device_id=(lax.rem(mx + step, nx), my), device_id_type=MESH,
        )

    def all_copy(kind, buffer, step):
        return pltpu.make_async_remote_copy(
            src_ref=buffer.at[me], dst_ref=buffer.at[me],
            send_sem=all_send.at[kind], recv_sem=all_recv.at[kind],
            device_id=place(lax.rem(me + step, n)), device_id_type=MESH,
        )

    def every(kind, buffer):
        whole = buffer.at[pl.ds(0, n - 1)]
        return pltpu.make_async_remote_copy(
            src_ref=whole, dst_ref=whole,
            send_sem=all_send.at[kind], recv_sem=all_recv.at[kind],
            device_id=place(lax.rem(me + 1, n)), device_id_type=MESH,
        )

    def send_all(kind, buffer):
        def one(step, carry):
            all_copy(kind, buffer, step).start()
            return carry

        lax.fori_loop(1, n, one, 0)

    dir_y[my] = direct
    for step in range(1, ny):
        y_copy(0, dir_y, step, False).start()

    for face in range(2, 4):
        recv_face(3, gap_ref.at[pl.ds((face - 2) * width, width)], gap_dst, face)
    far_gap = jnp.concatenate([masked(-gap_in[face - 2], face) for face in range(2, 4)], axis=0)
    spread = own_spread + wide_dot(scatter[:, 2 * width :], far_gap)
    weighted = (weight_all[...] * spread).astype(BF16)
    load_schur.wait()
    smoothed = jnp.dot(schur[...], weighted, preferred_element_type=F32)
    picks = wide_dot(gather[...], weight_all[...] * smoothed)
    measured = fine_dot(measure_rows, picks)
    for face in range(4):
        coarse_out[face] = measured[(face + 1) * MODE_ROWS : (face + 2) * MODE_ROWS]
    sum_y[my] = measured[5 * MODE_ROWS :]

    def coarse_dst(face):
        return coarse_in.at[face]

    def parts_dst(face):
        return parts_in.at[face]

    for face in range(4):
        send_face(4, coarse_out.at[face], coarse_dst, face)
    for step in range(1, ny):
        y_copy(1, sum_y, step, False).start()
    for face in range(4):
        parts[face] = picks[face * width : (face + 1) * width]
    for face in range(4):
        send_face(5, parts.at[face], parts_dst, face)

    energy_part = jnp.sum(own_gap * picks[: 2 * width], axis=0, keepdims=True) + jnp.sum(
        far_gap * picks[2 * width :], axis=0, keepdims=True
    )

    for face in range(4):
        recv_face(4, coarse_out.at[face], coarse_dst, face)
    coarse = measured[:MODE_ROWS]
    for face in range(4):
        coarse = coarse + jnp.where(present[face], coarse_in[face], 0.0)
    mode_at = lax.broadcasted_iota(jnp.int32, (SLOT_ROWS, cases), 0)
    all_coarse[me] = jnp.where(mode_at < modes, coarse[:SLOT_ROWS], energy_part)
    send_all(0, all_coarse)

    for kind, from_y, to_x in ((1, sum_y, sum_x), (0, dir_y, dir_x)):
        for step in range(1, ny):
            y_copy(kind, from_y, step, True).wait_recv()
        to_x[mx] = jnp.sum(from_y[...], axis=0)
        for step in range(1, nx):
            x_copy(kind, to_x, step, False).start()

    for face in range(4):
        recv_face(5, parts.at[face], parts_dst, face)
    opened = picks - jnp.concatenate([masked(parts_in[face], face) for face in range(4)], axis=0)

    for kind, to_x in ((0, dir_x), (1, sum_x)):
        for step in range(1, nx):
            x_copy(kind, to_x, step, True).wait_recv()
    coarse_rows = [inverse_pad[...]]
    coarse_rows += [jnp.where(present[face], inverse_in[face], 0.0) for face in range(4)]
    coarse_rows.append(jnp.sum(dir_x[...], axis=0))
    coarse_rows = jnp.concatenate(coarse_rows, axis=0)
    direct_sum = jnp.sum(sum_x[...], axis=0)
    every(0, all_coarse).wait_recv()
    gathered = all_coarse[...]
    energy = jnp.sum(gathered, axis=0)[modes : modes + 1]
    solved = fine_dot(coarse_rows, gathered.reshape(SLOT_ROWS * n, cases))
    factors = jnp.concatenate(
        [
            solved[: 5 * MODE_ROWS],
            direct_sum - solved[5 * MODE_ROWS :],
            jnp.zeros((128 - 5 * MODE_ROWS - ndir, cases), F32),
        ],
        axis=0,
    )
    high, low = split(factors)
    search = opened - jnp.dot(
        lift3, jnp.concatenate([high, low, high], axis=0), preferred_element_type=F32
    )

    lifted = wide_dot(scatter[...], search).astype(BF16)
    load_flex.wait()
    bent = jnp.dot(flex[...], lifted, preferred_element_type=F32)
    picks2 = wide_dot(gather[...], bent)
    all_curv[me] = jnp.sum(search * picks2, axis=0, keepdims=True)
    send_all(1, all_curv)
    for face in range(2):
        applied[face] = picks2[(face + 2) * width : (face + 3) * width]

    def applied_dst(face):
        return applied_in.at[face]

    for face in range(2, 4):
        send_face(6, applied.at[face - 2], applied_dst, face)
    for face in range(2):
        recv_face(6, applied.at[face], applied_dst, face)
    moved = picks2[: 2 * width] - jnp.concatenate(
        [masked(applied_in[face], face) for face in range(2)], axis=0
    )
    every(1, all_curv).wait_recv()
    curvature = jnp.sum(all_curv[...], axis=0)
    step_size = energy / curvature
    out_mult[...] = step_size * search[: 2 * width]
    out_res[...] = own_gap - step_size * moved

    for face in range(4):
        sent_face(0, modes_out.at[face], modes_dst, face)
        sent_face(1, inverse_pad, inverse_dst, face)
        sent_face(4, coarse_out.at[face], coarse_dst, face)
        sent_face(5, parts.at[face], parts_dst, face)
    for face in range(2):
        sent_face(2, kept_out.at[face], kept_dst, face)
        sent_face(3, gap_ref.at[pl.ds(face * width, width)], gap_dst, face)
    for face in range(2, 4):
        sent_face(6, applied.at[face - 2], applied_dst, face)
    for kind, y_buffer, x_buffer in ((0, dir_y, dir_x), (1, sum_y, sum_x)):
        for step in range(1, ny):
            y_copy(kind, y_buffer, step, False).wait_send()
        for step in range(1, nx):
            x_copy(kind, x_buffer, step, False).wait_send()
    every(0, all_coarse).wait_send()
    every(1, all_curv).wait_send()


def per_device(
    nx, ny, gap_load, flexibility, schur_blocks, body_modes, coarse_inverse, saved_search,
    saved_images, face_slots, face_count, multiplicity,
):
    n = nx * ny
    links2, cases = gap_load.shape[2:]
    width = links2 // 2
    modes, slot_total = body_modes.shape[2:]
    ndir = saved_search.shape[2]
    padded = SLOT_ROWS * n
    vmem = pl.BlockSpec(memory_space=pltpu.VMEM)
    hbm = pl.BlockSpec(memory_space=pl.ANY)
    smem = pl.BlockSpec(memory_space=pltpu.SMEM)
    dma = pltpu.SemaphoreType.DMA
    scratch = [
        pltpu.VMEM((slot_total, slot_total), BF16),
        pltpu.VMEM((slot_total, slot_total), BF16),
        pltpu.VMEM((4 * width, slot_total), BF16),
        pltpu.VMEM((slot_total, 4 * width), BF16),
        pltpu.VMEM((slot_total, cases), F32),
        pltpu.VMEM((MODE_ROWS, slot_total), F32),
        pltpu.VMEM((MODE_ROWS, modes * n), F32),
        pltpu.VMEM((4, MODE_ROWS, width), F32),
        pltpu.VMEM((4, MODE_ROWS, width), F32),
        pltpu.VMEM((MODE_ROWS, padded), F32),
        pltpu.VMEM((4, MODE_ROWS, padded), F32),
        pltpu.VMEM((2, 2 * ndir, width), F32),
        pltpu.VMEM((2, 2 * ndir, width), F32),
        pltpu.VMEM((2, width, cases), F32),
        pltpu.VMEM((4, width, cases), F32),
        pltpu.VMEM((4, width, cases), F32),
        pltpu.VMEM((4, MODE_ROWS, cases), F32),
        pltpu.VMEM((4, MODE_ROWS, cases), F32),
        pltpu.VMEM((n, SLOT_ROWS, cases), F32),
        pltpu.VMEM((ny, ndir, cases), F32),
        pltpu.VMEM((nx, ndir, cases), F32),
        pltpu.VMEM((ny, ndir, padded), F32),
        pltpu.VMEM((nx, ndir, padded), F32),
        pltpu.VMEM((n, 1, cases), F32),
        pltpu.VMEM((2, width, cases), F32),
        pltpu.VMEM((2, width, cases), F32),
        dma((2,)),
        dma((7, 4)),
        dma((7, 4)),
        dma((2, ny)),
        dma((2, ny)),
        dma((2, nx)),
        dma((2, nx)),
        dma((2,)),
        dma((2,)),
    ]
    out = jax.ShapeDtypeStruct((links2, cases), F32)
    multipliers, residual = pl.pallas_call(
        functools.partial(kernel, nx, ny),
        out_shape=(out, out),
        in_specs=[vmem, hbm, hbm, vmem, vmem, vmem, vmem, vmem, smem, vmem],
        out_specs=(vmem, vmem),
        scratch_shapes=scratch,
        compiler_params=pltpu.CompilerParams(
            collective_id=0, has_side_effects=True, vmem_limit_bytes=48 * 1024 * 1024
        ),
    )(
        gap_load[0, 0], flexibility[0, 0], schur_blocks[0, 0], body_modes[0, 0], coarse_inverse,
        saved_search[0, 0], saved_images[0, 0], face_slots[0, 0], face_count[0], multiplicity[0],
    )
    return (multipliers[None, None], residual[None, None])


def solution(mesh):
    in_specs = (
        P("gx", "gy", None, None),
        P("gx", "gy", None, None),
        P("gx", "gy", None, None),
        P("gx", "gy", None, None),
        P(("gx", "gy"), None),
        P("gx", "gy", None, None),
        P("gx", "gy", None, None),
        P("gx", "gy", None, None),
        P("gx", "gy", None),
        P("gx", "gy", None),
    )
    out_specs = (P("gx", "gy", None, None), P("gx", "gy", None, None))
    return jax.shard_map(
        functools.partial(per_device, mesh.shape["gx"], mesh.shape["gy"]),
        mesh=mesh, in_specs=in_specs, out_specs=out_specs, check_vma=False,
    )
```

```python
import functools

import jax
import jax.numpy as jnp
from jax import lax
from jax.experimental import pallas as pl
from jax.experimental.pallas import tpu as pltpu
from jax.sharding import PartitionSpec as P

HIGHEST_MODE = lax.Precision.HIGHEST
MESH = pl.DeviceIdType.MESH
F32 = jnp.float32
BF16 = jnp.bfloat16
FACE_ROWS = (1, 3, 0, 2)
MODE_ROWS = 8
SLOT_ROWS = 4


def split(value):
    high = value.astype(BF16)
    return high, (value - high.astype(F32)).astype(BF16)


def wide_dot(one_hot, value):
    width = value.shape[1]
    both = jnp.concatenate(split(value), axis=1)
    out = jnp.dot(one_hot, both, preferred_element_type=F32)
    return out[:, :width] + out[:, width:]


def full_dot(one_hot, value):
    high, low = split(value)
    last = ((value - high.astype(F32)) - low.astype(F32)).astype(BF16)
    width = value.shape[1]
    out = jnp.dot(one_hot, jnp.concatenate([high, low, last], axis=1), preferred_element_type=F32)
    return out[:, :width] + (out[:, width : 2 * width] + out[:, 2 * width :])


def fine_dot(left, right):
    rows, width = left.shape[0], right.shape[1]
    lefts = jnp.concatenate(split(left), axis=0)
    rights = jnp.concatenate(split(right), axis=1)
    out = jnp.dot(lefts, rights, preferred_element_type=F32)
    return (out[:rows, :width] + out[rows:, :width]) + (out[:rows, width:] + out[rows:, width:])


def kernel(
    nx, ny,
    gap_hbm, flex_hbm, schur_hbm, modes_hbm, inverse_hbm, search_hbm, images_hbm, slots_hbm,
    count_hbm, mult_hbm,
    out_mult, out_res,
    gap_ref, modes_ref, inverse_ref, search_ref, images_ref, slots_ref, count_ref, mult_ref,
    flex, schur, gather, scatter, weight_all, modes8, inverse8, modes_out, modes_in,
    inverse_pad, inverse_in, kept_out, kept_in, gap_in, parts, parts_in, coarse_out, coarse_in,
    all_coarse, sum_y, sum_x, dir_y, dir_x, all_curv, applied, applied_in,
    load_sem, face_send, face_recv, y_send, y_recv, x_send, x_recv, all_send, all_recv,
):
    n = nx * ny
    mx = lax.axis_index("gx")
    my = lax.axis_index("gy")
    me = mx * ny + my
    slot_total = mult_ref.shape[1]
    width = slots_ref.shape[1]
    cases = gap_ref.shape[1]
    ndir = search_ref.shape[0]
    links = 4 * width
    modes = modes_ref.shape[0]
    present = (mx < nx - 1, my < ny - 1, mx > 0, my > 0)
    beside = ((mx + 1, my), (mx, my + 1), (mx - 1, my), (mx, my - 1))

    def place(index):
        return (index // ny, lax.rem(index, ny))

    loads = [
        pltpu.make_async_copy(source, target, load_sem.at[at])
        for at, (source, target) in enumerate(
            (
                (count_hbm, count_ref), (slots_hbm, slots_ref), (modes_hbm, modes_ref),
                (inverse_hbm, inverse_ref), (search_hbm, search_ref), (images_hbm, images_ref),
                (mult_hbm, mult_ref), (gap_hbm, gap_ref), (schur_hbm, schur), (flex_hbm, flex),
            )
        )
    ]
    for load in loads:
        load.start()
    load_schur, load_flex = loads[8:]

    barrier = pltpu.get_barrier_semaphore()

    def greet(step, carry):
        pl.semaphore_signal(
            barrier, inc=1, device_id=place(lax.rem(me + step, n)), device_id_type=MESH
        )
        return carry

    lax.fori_loop(1, n, greet, 0)

    def face_copy(kind, src, dst_of, face, arriving):
        landing = face if arriving else (face + 2) % 4
        return pltpu.make_async_remote_copy(
            src_ref=src, dst_ref=dst_of(landing),
            send_sem=face_send.at[kind, face], recv_sem=face_recv.at[kind, landing],
            device_id=beside[face], device_id_type=MESH,
        )

    def send_face(kind, src, dst_of, face):
        @pl.when(present[face])
        def _():
            face_copy(kind, src, dst_of, face, False).start()

    def recv_face(kind, src, dst_of, face):
        @pl.when(present[face])
        def _():
            face_copy(kind, src, dst_of, face, True).wait_recv()

    def sent_face(kind, src, dst_of, face):
        @pl.when(present[face])
        def _():
            face_copy(kind, src, dst_of, face, False).wait_send()

    for load in loads[:8]:
        load.wait()

    def count_of(face):
        return count_ref[:, FACE_ROWS[face] : FACE_ROWS[face] + 1]

    def row_of(face):
        row = slots_ref[FACE_ROWS[face] : FACE_ROWS[face] + 1, :]
        at = lax.broadcasted_iota(jnp.int32, (1, width), 1)
        return jnp.where(at < count_of(face), row, -1).astype(F32)

    slot_row = jnp.concatenate([row_of(face) for face in range(4)], axis=1)
    slot_at = lax.broadcasted_iota(jnp.int32, (slot_total, links), 0).astype(F32)
    scatter[...] = jnp.where(slot_at == slot_row, 1.0, 0.0).astype(BF16)

    modes8[...] = jnp.zeros_like(modes8)
    for mode in range(modes):
        modes8[mode : mode + 1, :] = modes_ref[mode]
    mode_parts = jnp.concatenate(split(modes8[...]), axis=0)
    rest = modes8[...] - mode_parts[:MODE_ROWS].astype(F32) - mode_parts[MODE_ROWS:].astype(F32)
    mode_parts = jnp.concatenate(
        [mode_parts[:MODE_ROWS].astype(F32), mode_parts[MODE_ROWS:].astype(F32), rest], axis=0
    ).astype(BF16)
    picked3 = jnp.dot(mode_parts, scatter[...], preferred_element_type=F32)
    picked_modes = (
        picked3[:MODE_ROWS] + picked3[MODE_ROWS : 2 * MODE_ROWS] + picked3[2 * MODE_ROWS :]
    )
    for face in range(4):
        modes_out[face] = picked_modes[:, face * width : (face + 1) * width]

    inverse8[...] = jnp.zeros_like(inverse8)
    inverse8[0:modes, :] = inverse_ref[...]
    chunk = min(n, 32)
    from_at = lax.broadcasted_iota(jnp.int32, (modes * chunk, SLOT_ROWS * chunk), 0)
    to_at = lax.broadcasted_iota(jnp.int32, (modes * chunk, SLOT_ROWS * chunk), 1)
    inner = to_at % SLOT_ROWS
    expand = jnp.where((inner < modes) & (from_at == (to_at // SLOT_ROWS) * modes + inner), 1.0, 0.0)
    for at in range(n // chunk):
        inverse_pad[:, at * SLOT_ROWS * chunk : (at + 1) * SLOT_ROWS * chunk] = jnp.dot(
            inverse8[:, at * modes * chunk : (at + 1) * modes * chunk], expand,
            precision=HIGHEST_MODE, preferred_element_type=F32,
        )

    for face in range(2):
        kept_out[face, 0:ndir, :] = search_ref[:, face * width : (face + 1) * width]
        kept_out[face, ndir:, :] = images_ref[:, face * width : (face + 1) * width]

    pl.semaphore_wait(barrier, n - 1)

    def modes_dst(face):
        return modes_in.at[face]

    def inverse_dst(face):
        return inverse_in.at[face]

    def kept_dst(face):
        return kept_in.at[face - 2]

    def gap_dst(face):
        return gap_in.at[face - 2]

    for face in range(2):
        send_face(2, kept_out.at[face], kept_dst, face)
        send_face(0, modes_out.at[face], modes_dst, face)
        send_face(1, inverse_pad, inverse_dst, face)
        send_face(3, gap_ref.at[pl.ds(face * width, width)], gap_dst, face)
    for face in range(2, 4):
        send_face(0, modes_out.at[face], modes_dst, face)
        send_face(1, inverse_pad, inverse_dst, face)

    columns = jnp.transpose(jnp.broadcast_to(slot_row, (128, links)))
    lane = lax.broadcasted_iota(jnp.int32, (links, 128), 1).astype(F32)
    for at in range(slot_total // 128):
        gather[:, at * 128 : (at + 1) * 128] = jnp.where(
            columns == lane + float(at * 128), 1.0, 0.0
        ).astype(BF16)
    weight_row = 1.0 / mult_ref[...].astype(F32)
    weight_all[...] = jnp.transpose(jnp.broadcast_to(weight_row, (cases, slot_total)))

    row_at = lax.broadcasted_iota(jnp.int32, (width, cases), 0)

    def masked(value, face):
        return jnp.where(row_at < count_of(face), value, 0.0)

    own_gap = jnp.concatenate(
        [masked(gap_ref[face * width : (face + 1) * width, :], face) for face in range(2)], axis=0
    )
    own_spread = full_dot(scatter[:, : 2 * width], own_gap)

    for face in range(4):
        recv_face(0, modes_out.at[face], modes_dst, face)
        recv_face(1, inverse_pad, inverse_dst, face)
    for face in range(2, 4):
        recv_face(2, kept_out.at[face - 2], kept_dst, face)

    def lanes_masked(value, face):
        at = lax.broadcasted_iota(jnp.int32, value.shape, 1)
        return jnp.where(at < count_of(face), value, 0.0)

    near = jnp.concatenate([lanes_masked(-modes_in[face], face) for face in range(4)], axis=1)
    at = lax.broadcasted_iota(jnp.int32, near.shape, 1)
    blocks = [picked_modes]
    for face in range(4):
        blocks.append(jnp.where((at >= face * width) & (at < (face + 1) * width), near, 0.0))
    mode_rows = jnp.concatenate(blocks, axis=0)
    kept = [lanes_masked(kept_out[face], face) for face in range(2)]
    kept += [lanes_masked(-kept_in[face - 2], face) for face in range(2, 4)]
    kept = jnp.concatenate(kept, axis=1)
    kept_search, kept_images = kept[:ndir], kept[ndir:]
    measure_rows = jnp.concatenate([mode_rows, kept_images], axis=0)
    filler = jnp.zeros((128 - 5 * MODE_ROWS - ndir, links), F32)
    lift = jnp.transpose(jnp.concatenate([mode_rows, kept_search, filler], axis=0))
    lift_high, lift_low = split(lift)
    lift3 = jnp.concatenate([lift_high, lift_high, lift_low], axis=1)

    own_part = lax.dot_general(
        kept_images, picked_modes, (((1,), (1,)), ((), ())),
        precision=HIGHEST_MODE, preferred_element_type=F32,
    )
    direct = jnp.dot(
        own_part, inverse_pad[...], precision=HIGHEST_MODE, preferred_element_type=F32
    )

    def y_copy(kind, buffer, step, arriving):
        slot = lax.rem(my - step + ny, ny) if arriving else my
        return pltpu.make_async_remote_copy(
            src_ref=buffer.at[my], dst_ref=buffer.at[slot],
            send_sem=y_send.at[kind, step], recv_sem=y_recv.at[kind, step],
            device_id=(mx, lax.rem(my + step, ny)), device_id_type=MESH,
        )

    def x_copy(kind, buffer, step, arriving):
        slot = lax.rem(mx - step + nx, nx) if arriving else mx
        return pltpu.make_async_remote_copy(
            src_ref=buffer.at[mx], dst_ref=buffer.at[slot],
            send_sem=x_send.at[kind, step], recv_sem=x_recv.at[kind, step],
            device_id=(lax.rem(mx + step, nx), my), device_id_type=MESH,
        )

    def all_copy(kind, buffer, step):
        return pltpu.make_async_remote_copy(
            src_ref=buffer.at[me], dst_ref=buffer.at[me],
            send_sem=all_send.at[kind], recv_sem=all_recv.at[kind],
            device_id=place(lax.rem(me + step, n)), device_id_type=MESH,
        )

    def every(kind, buffer):
        whole = buffer.at[pl.ds(0, n - 1)]
        return pltpu.make_async_remote_copy(
            src_ref=whole, dst_ref=whole,
            send_sem=all_send.at[kind], recv_sem=all_recv.at[kind],
            device_id=place(lax.rem(me + 1, n)), device_id_type=MESH,
        )

    def send_all(kind, buffer):
        def one(step, carry):
            all_copy(kind, buffer, step).start()
            return carry

        lax.fori_loop(1, n, one, 0)

    dir_y[my] = direct
    for step in range(1, ny):
        y_copy(0, dir_y, step, False).start()

    for face in range(2, 4):
        recv_face(3, gap_ref.at[pl.ds((face - 2) * width, width)], gap_dst, face)
    far_gap = jnp.concatenate([masked(-gap_in[face - 2], face) for face in range(2, 4)], axis=0)
    spread = own_spread + full_dot(scatter[:, 2 * width :], far_gap)
    weighted = (weight_all[...] * spread).astype(BF16)
    load_schur.wait()
    smoothed = jnp.dot(schur[...], weighted, preferred_element_type=F32)
    picks = full_dot(gather[...], weight_all[...] * smoothed)
    measured = fine_dot(measure_rows, picks)
    for face in range(4):
        coarse_out[face] = measured[(face + 1) * MODE_ROWS : (face + 2) * MODE_ROWS]
    sum_y[my] = measured[5 * MODE_ROWS :]

    def coarse_dst(face):
        return coarse_in.at[face]

    def parts_dst(face):
        return parts_in.at[face]

    for face in range(4):
        send_face(4, coarse_out.at[face], coarse_dst, face)
    for step in range(1, ny):
        y_copy(1, sum_y, step, False).start()
    for face in range(4):
        parts[face] = picks[face * width : (face + 1) * width]
    for face in range(4):
        send_face(5, parts.at[face], parts_dst, face)

    energy_part = jnp.sum(own_gap * picks[: 2 * width], axis=0, keepdims=True) + jnp.sum(
        far_gap * picks[2 * width :], axis=0, keepdims=True
    )

    for face in range(4):
        recv_face(4, coarse_out.at[face], coarse_dst, face)
    coarse = measured[:MODE_ROWS]
    for face in range(4):
        coarse = coarse + jnp.where(present[face], coarse_in[face], 0.0)
    mode_at = lax.broadcasted_iota(jnp.int32, (SLOT_ROWS, cases), 0)
    all_coarse[me] = jnp.where(mode_at < modes, coarse[:SLOT_ROWS], energy_part)
    send_all(0, all_coarse)

    for kind, from_y, to_x in ((1, sum_y, sum_x), (0, dir_y, dir_x)):
        for step in range(1, ny):
            y_copy(kind, from_y, step, True).wait_recv()
        to_x[mx] = jnp.sum(from_y[...], axis=0)
        for step in range(1, nx):
            x_copy(kind, to_x, step, False).start()

    for face in range(4):
        recv_face(5, parts.at[face], parts_dst, face)
    opened = picks - jnp.concatenate([masked(parts_in[face], face) for face in range(4)], axis=0)

    for kind, to_x in ((0, dir_x), (1, sum_x)):
        for step in range(1, nx):
            x_copy(kind, to_x, step, True).wait_recv()
    coarse_rows = [inverse_pad[...]]
    coarse_rows += [jnp.where(present[face], inverse_in[face], 0.0) for face in range(4)]
    coarse_rows.append(jnp.sum(dir_x[...], axis=0))
    coarse_rows = jnp.concatenate(coarse_rows, axis=0)
    direct_sum = jnp.sum(sum_x[...], axis=0)
    every(0, all_coarse).wait_recv()
    gathered = all_coarse[...]
    energy = jnp.sum(gathered, axis=0)[modes : modes + 1]
    solved = fine_dot(coarse_rows, gathered.reshape(SLOT_ROWS * n, cases))
    factors = jnp.concatenate(
        [
            solved[: 5 * MODE_ROWS],
            direct_sum - solved[5 * MODE_ROWS :],
            jnp.zeros((128 - 5 * MODE_ROWS - ndir, cases), F32),
        ],
        axis=0,
    )
    high, low = split(factors)
    search = opened - jnp.dot(
        lift3, jnp.concatenate([high, low, high], axis=0), preferred_element_type=F32
    )

    lifted = full_dot(scatter[...], search).astype(BF16)
    load_flex.wait()
    bent = jnp.dot(flex[...], lifted, preferred_element_type=F32)
    picks2 = wide_dot(gather[...], bent)
    all_curv[me] = jnp.sum(search * picks2, axis=0, keepdims=True)
    send_all(1, all_curv)
    for face in range(2):
        applied[face] = picks2[(face + 2) * width : (face + 3) * width]

    def applied_dst(face):
        return applied_in.at[face]

    for face in range(2, 4):
        send_face(6, applied.at[face - 2], applied_dst, face)
    for face in range(2):
        recv_face(6, applied.at[face], applied_dst, face)
    moved = picks2[: 2 * width] - jnp.concatenate(
        [masked(applied_in[face], face) for face in range(2)], axis=0
    )
    every(1, all_curv).wait_recv()
    curvature = jnp.sum(all_curv[...], axis=0)
    step_size = energy / curvature
    out_mult[...] = step_size * search[: 2 * width]
    out_res[...] = own_gap - step_size * moved

    for face in range(4):
        sent_face(0, modes_out.at[face], modes_dst, face)
        sent_face(1, inverse_pad, inverse_dst, face)
        sent_face(4, coarse_out.at[face], coarse_dst, face)
        sent_face(5, parts.at[face], parts_dst, face)
    for face in range(2):
        sent_face(2, kept_out.at[face], kept_dst, face)
        sent_face(3, gap_ref.at[pl.ds(face * width, width)], gap_dst, face)
    for face in range(2, 4):
        sent_face(6, applied.at[face - 2], applied_dst, face)
    for kind, y_buffer, x_buffer in ((0, dir_y, dir_x), (1, sum_y, sum_x)):
        for step in range(1, ny):
            y_copy(kind, y_buffer, step, False).wait_send()
        for step in range(1, nx):
            x_copy(kind, x_buffer, step, False).wait_send()
    every(0, all_coarse).wait_send()
    every(1, all_curv).wait_send()


def per_device(
    nx, ny, gap_load, flexibility, schur_blocks, body_modes, coarse_inverse, saved_search,
    saved_images, face_slots, face_count, multiplicity,
):
    n = nx * ny
    links2, cases = gap_load.shape[2:]
    width = links2 // 2
    modes, slot_total = body_modes.shape[2:]
    ndir = saved_search.shape[2]
    padded = SLOT_ROWS * n
    vmem = pl.BlockSpec(memory_space=pltpu.VMEM)
    hbm = pl.BlockSpec(memory_space=pl.ANY)
    dma = pltpu.SemaphoreType.DMA
    scratch = [
        pltpu.VMEM((links2, cases), F32),
        pltpu.VMEM((modes, 1, slot_total), F32),
        pltpu.VMEM((modes, modes * n), F32),
        pltpu.VMEM((ndir, links2), F32),
        pltpu.VMEM((ndir, links2), F32),
        pltpu.VMEM((4, width), jnp.int32),
        pltpu.VMEM((1, 4), jnp.int32),
        pltpu.VMEM((1, slot_total), jnp.int32),
        pltpu.VMEM((slot_total, slot_total), BF16),
        pltpu.VMEM((slot_total, slot_total), BF16),
        pltpu.VMEM((4 * width, slot_total), BF16),
        pltpu.VMEM((slot_total, 4 * width), BF16),
        pltpu.VMEM((slot_total, cases), F32),
        pltpu.VMEM((MODE_ROWS, slot_total), F32),
        pltpu.VMEM((MODE_ROWS, modes * n), F32),
        pltpu.VMEM((4, MODE_ROWS, width), F32),
        pltpu.VMEM((4, MODE_ROWS, width), F32),
        pltpu.VMEM((MODE_ROWS, padded), F32),
        pltpu.VMEM((4, MODE_ROWS, padded), F32),
        pltpu.VMEM((2, 2 * ndir, width), F32),
        pltpu.VMEM((2, 2 * ndir, width), F32),
        pltpu.VMEM((2, width, cases), F32),
        pltpu.VMEM((4, width, cases), F32),
        pltpu.VMEM((4, width, cases), F32),
        pltpu.VMEM((4, MODE_ROWS, cases), F32),
        pltpu.VMEM((4, MODE_ROWS, cases), F32),
        pltpu.VMEM((n, SLOT_ROWS, cases), F32),
        pltpu.VMEM((ny, ndir, cases), F32),
        pltpu.VMEM((nx, ndir, cases), F32),
        pltpu.VMEM((ny, ndir, padded), F32),
        pltpu.VMEM((nx, ndir, padded), F32),
        pltpu.VMEM((n, 1, cases), F32),
        pltpu.VMEM((2, width, cases), F32),
        pltpu.VMEM((2, width, cases), F32),
        dma((10,)),
        dma((7, 4)),
        dma((7, 4)),
        dma((2, ny)),
        dma((2, ny)),
        dma((2, nx)),
        dma((2, nx)),
        dma((2,)),
        dma((2,)),
    ]
    out = jax.ShapeDtypeStruct((links2, cases), F32)
    multipliers, residual = pl.pallas_call(
        functools.partial(kernel, nx, ny),
        out_shape=(out, out),
        in_specs=[hbm] * 10,
        out_specs=(vmem, vmem),
        scratch_shapes=scratch,
        compiler_params=pltpu.CompilerParams(
            collective_id=0, has_side_effects=True
        ),
    )(
        gap_load[0, 0], flexibility[0, 0], schur_blocks[0, 0], jnp.reshape(body_modes, (modes, 1, slot_total)), coarse_inverse,
        saved_search[0, 0], saved_images[0, 0], face_slots[0, 0], face_count[0], multiplicity[0],
    )
    return (multipliers[None, None], residual[None, None])


def solution(mesh):
    in_specs = (
        P("gx", "gy", None, None),
        P("gx", "gy", None, None),
        P("gx", "gy", None, None),
        P("gx", "gy", None, None),
        P(("gx", "gy"), None),
        P("gx", "gy", None, None),
        P("gx", "gy", None, None),
        P("gx", "gy", None, None),
        P("gx", "gy", None),
        P("gx", "gy", None),
    )
    out_specs = (P("gx", "gy", None, None), P("gx", "gy", None, None))
    return jax.shard_map(
        functools.partial(per_device, mesh.shape["gx"], mesh.shape["gy"]),
        mesh=mesh, in_specs=in_specs, out_specs=out_specs, check_vma=False,
    )
```
